32 devices in a mesh: section: 4 (over z), dom: 8 (over y, x, core).
Axes of the slice: x: 2, y: 2, z: 4, core: 2. Of those that a mesh axis runs over, the one named last changes fastest.
Arguments:
- layer_inputs: bfloat16 [4, 16384, 512], P('section', 'dom'), may hold values from -6 to 6
- adjacency: bfloat16 [128, 8, 128, 128], P('dom'), may hold values from -0.1875 to 0.1875
- columns: int32 [128, 8], P('dom'), may hold values from 0 to 127, as said below
- group_order: int32 [8, 4], P('dom'), may hold values from 0 to 3, each once within a row
- weights: bfloat16 [4, 512, 512], P('section'), may hold values from -0.25 to 0.25
Outputs:
- embeddings: bfloat16 [4, 16384, 512], P('section', 'dom')
The draws below stay inside these ranges and needn't reach their ends.
Inputs may be any that keep to these rules, and one draw needn't show every extreme that they name: `columns`: the tiles of a row block of part p name row blocks of parts p - 1, p and p + 1, counted modulo 8. `group_order`: each row is a permutation.
All inputs are finite; a program needn't handle non-finite values.
Results may differ from the reference program's by a relative error of at most 0.0095.
Values may be sent and summed in bfloat16 or wider, within the bound.
A program may use at most 64 MiB of HBM per device.

```python
import jax
import jax.numpy as jnp
from jax import lax

D = 512
BLOCK = 128
TILES = 8
GROUPS = 4
LAYERS = 4
PARTS_SIZE = 8
NODES = 16384
NBLK = 128
BPP = 16


def draw_columns(key, part):
    first_key, second_key = jax.random.split(jax.random.fold_in(key, 17))
    offsets = jax.random.randint(first_key, (NBLK, TILES), 0, 3) - 1
    inside = jax.random.randint(second_key, (NBLK, TILES), 0, BPP)
    owners = (jnp.arange(NBLK, dtype=jnp.int32) // BPP)[:, None]
    return ((owners + offsets) % PARTS_SIZE * BPP + inside).astype(jnp.int32)


def block_scale(key, dims, pieces, low, top_value):
    factor_of = 1.0
    for dim, blocks in pieces:
        draws = jax.random.uniform(jax.random.fold_in(jax.random.fold_in(key, 6), dim), (blocks,), jnp.float32, low / len(pieces), top_value / len(pieces))
        factor_of = factor_of * jnp.repeat(jnp.exp(draws), dims[dim] // blocks).reshape((-1,) + (1,) * (len(dims) - 1 - dim))
    return factor_of


def centred(own_key, dims, scale, bound, shards=(), held_as=jnp.bfloat16):
    factor_of = block_scale(own_key, dims, shards, -0.22, 0.18) if shards else 1.0
    array = jax.random.normal(own_key, dims, jnp.float32) * scale * factor_of
    return jnp.minimum(jnp.maximum(array, -bound), bound).astype(held_as)


def setup_inputs(seed: int = 0) -> dict:
    keys = jax.random.split(jax.random.key(seed), 6)
    layer_inputs = centred(keys[0], (LAYERS, NODES, D), 1.0, 6.0, ((0, 4), (1, 8)))
    adjacency = centred(keys[1], (NBLK, TILES, BLOCK, BLOCK), (TILES * BLOCK) ** -0.5, 0.1875, ((0, 8),))
    columns = draw_columns(jax.random.fold_in(keys[5], 71), 0)
    group_order = jax.vmap(lambda own: jax.random.permutation(own, GROUPS))(jax.random.split(keys[3], PARTS_SIZE)).reshape((PARTS_SIZE, GROUPS)).astype(jnp.int32)
    weights = centred(keys[4], (LAYERS, D, D), D ** -0.5, 0.25, ((0, 4),))
    return dict(layer_inputs=layer_inputs, adjacency=adjacency, columns=columns, group_order=group_order, weights=weights)


def reference(layer_inputs, adjacency, columns, group_order, weights):
    part_count = group_order.shape[0]
    blocks_part = adjacency.shape[0] // part_count
    blocks_group = blocks_part // GROUPS
    positions = jnp.arange(GROUPS, dtype=jnp.int32)
    matches = group_order[:, :, None] == positions[None, None, :]
    group_step = jnp.sum(jnp.where(matches, positions[None, :, None], 0), axis=1).astype(jnp.int32)
    block_ids = jnp.arange(NBLK, dtype=jnp.int32)
    block_step = group_step[block_ids // blocks_part, (block_ids % blocks_part) // blocks_group]
    fresh_mask = block_step[columns] <= block_step[:, None]
    tile_parts = adjacency.reshape(part_count, blocks_part, TILES, BLOCK, BLOCK)
    column_parts = columns.reshape(part_count, blocks_part, TILES)
    fresh_parts = fresh_mask.reshape(part_count, blocks_part, TILES)
    current = layer_inputs[0]
    results = []
    for layer_index in range(LAYERS):
        current_blocks = current.reshape(NBLK, BLOCK, D)
        stale_blocks = layer_inputs[layer_index].reshape(NBLK, BLOCK, D)

        def per_part(packed):
            tile_part, column_part, fresh_part = packed
            sources = jnp.where(fresh_part[:, :, None, None], current_blocks[column_part], stale_blocks[column_part])
            summed = jnp.einsum('rkij,rkjd->rid', tile_part.astype(jnp.float32), sources.astype(jnp.float32))
            return summed.astype(jnp.bfloat16)

        aggregate = lax.map(per_part, (tile_parts, column_parts, fresh_parts)).reshape(NODES, D)
        product = jnp.dot(aggregate, weights[layer_index], preferred_element_type=jnp.float32)
        current = (current.astype(jnp.float32) + jax.nn.relu(product)).astype(jnp.bfloat16)
        results.append(current)
    return jnp.stack(results)
```

```python
import functools

import jax
import jax.numpy as jnp
from jax import lax
from jax.experimental import pallas as pl
from jax.experimental.pallas import tpu as pltpu
from jax.sharding import PartitionSpec as P

MESH = pl.DeviceIdType.MESH


def pipeline_kernel(
    sections, parts, groups, table, order, x_ref, adj_hbm, w_ref, out_ref,
    adj, src, mine, own_land, side_land,
    adj_sem, stale_send, stale_recv, z_send, z_recv, f_send, f_recv,
):
    s = lax.axis_index("section")
    d = lax.axis_index("dom")
    right, left = lax.rem(d + 1, parts), lax.rem(d + parts - 1, parts)
    blocks, side, width = x_ref.shape
    tiles = adj.shape[1]
    bg = blocks // groups
    fresh = 3 * blocks
    last = sections - 1

    load_adj = pltpu.make_async_copy(adj_hbm, adj, adj_sem)
    load_adj.start()

    for k in range(groups):
        piece = x_ref[pl.ds(order[k] * bg, bg)]
        mine[k * bg:(k + 1) * bg] = piece
        src[blocks + k * bg:blocks + (k + 1) * bg] = piece

    barrier = pltpu.get_barrier_semaphore()
    for neighbour in (left, right):
        pl.semaphore_signal(barrier, inc=1, device_id={"dom": neighbour}, device_id_type=MESH)

    @pl.when(s > 0)
    def _():
        pl.semaphore_signal(barrier, inc=1, device_id={"section": s - 1}, device_id_type=MESH)

    @pl.when(s < last)
    def _():
        pl.semaphore_signal(barrier, inc=1, device_id={"section": s + 1}, device_id_type=MESH)

    peers = 2 + jnp.where(s > 0, 1, 0) + jnp.where(s < last, 1, 0)
    pl.semaphore_wait(barrier, peers)

    def stale_copy(way, k):
        base = (0 if way == 0 else 2 * blocks) + k * bg
        return pltpu.make_async_remote_copy(
            src_ref=mine.at[pl.ds(k * bg, bg)],
            dst_ref=src.at[pl.ds(base, bg)],
            send_sem=stale_send.at[way, k],
            recv_sem=stale_recv.at[way, k],
            device_id={"dom": right if way == 0 else left},
            device_id_type=MESH,
        )

    def side_copy(way, r):
        return pltpu.make_async_remote_copy(
            src_ref=own_land.at[r],
            dst_ref=side_land.at[way, r],
            send_sem=f_send.at[way, r],
            recv_sem=f_recv.at[way, r],
            device_id={"dom": right if way == 0 else left},
            device_id_type=MESH,
        )

    def up_copy(r):
        return pltpu.make_async_remote_copy(
            src_ref=out_ref.at[r],
            dst_ref=own_land.at[r],
            send_sem=z_send.at[r],
            recv_sem=z_recv.at[r],
            device_id={"section": jnp.minimum(s + 1, last)},
            device_id_type=MESH,
        )

    @pl.when(s == 0)
    def _():
        for way in range(2):
            stale_copy(way, 0).start()

    for k in range(1, groups):
        for way in range(2):
            stale_copy(way, k).start()

    load_adj.wait()
    own_base = jnp.where(s > 0, fresh + blocks, blocks)

    for k in range(groups):
        lo, hi = k * bg, (k + 1) * bg

        @pl.when(s > 0)
        def _():
            @pl.loop(lo, hi)
            def _(r):
                up_copy(r).wait_recv()
                side_copy(0, r).start()
                side_copy(1, r).start()

            src[fresh + blocks + lo:fresh + blocks + hi] = own_land[lo:hi]

            @pl.loop(lo, hi)
            def _(r):
                side_copy(0, r).wait_recv()
                side_copy(1, r).wait_recv()

            src[fresh + lo:fresh + hi] = side_land[0, lo:hi]
            src[fresh + 2 * blocks + lo:fresh + 2 * blocks + hi] = side_land[1, lo:hi]

        if k == 0:
            @pl.when(s == 0)
            def _():
                for way in range(2):
                    stale_copy(way, 0).wait_recv()

            for q in range(1, groups):
                for way in range(2):
                    stale_copy(way, q).wait_recv()

        @pl.loop(lo, hi)
        def _(r):
            row = order[k] * bg + (r - lo)
            a = jnp.concatenate([adj[row, t] for t in range(tiles)], axis=1)
            h = jnp.concatenate([src[table[r * tiles + t]] for t in range(tiles)], axis=0)
            agg = jnp.dot(a, h, preferred_element_type=jnp.float32).astype(jnp.bfloat16)
            product = jnp.dot(agg, w_ref[...], preferred_element_type=jnp.float32)
            before = src[own_base + r].astype(jnp.float32)
            out_ref[r] = (before + jnp.maximum(product, 0.0)).astype(jnp.bfloat16)

            @pl.when(s < last)
            def _():
                up_copy(r).start()

    for k in range(1, groups):
        for way in range(2):
            stale_copy(way, k).wait_send()

    @pl.when(s == 0)
    def _():
        for way in range(2):
            stale_copy(way, 0).wait_send()

    @pl.when(s > 0)
    def _():
        @pl.loop(0, blocks)
        def _(r):
            side_copy(0, r).wait_send()
            side_copy(1, r).wait_send()

    @pl.when(s < last)
    def _():
        @pl.loop(0, blocks)
        def _(r):
            up_copy(r).wait_send()


def place_kernel(where, h_ref, out_ref):
    out_ref[...] = h_ref[...]


def on_device(sections, layer_inputs, adjacency, columns, group_order, weights):
    parts = lax.axis_size("dom")
    d = lax.axis_index("dom")
    s = lax.axis_index("section")
    rows, width = layer_inputs.shape[1:]
    blocks, tiles, side = adjacency.shape[:3]
    groups = group_order.shape[1]
    bg = blocks // groups
    up = [(i, (i + 1) % parts) for i in range(parts)]
    down = [(j, i) for i, j in up]
    before = lax.ppermute(group_order, "dom", up)
    after = lax.ppermute(group_order, "dom", down)
    orders = jnp.concatenate([before, group_order, after], axis=0)
    ids = jnp.arange(groups, dtype=jnp.int32)
    position = jnp.sum(
        jnp.where(orders[:, :, None] == ids[None, None, :], ids[None, :, None], 0), axis=1
    ).astype(jnp.int32)
    relative = (columns // blocks - d + 1) % parts
    inside = columns % blocks
    key = relative * groups + inside // bg
    flat = position.reshape(-1)
    hits = key[:, :, None] == jnp.arange(3 * groups, dtype=jnp.int32)[None, None, :]
    tile_pos = jnp.sum(jnp.where(hits, flat[None, None, :], 0), axis=2)
    row_pos = jnp.repeat(position[1], bg)
    is_fresh = (tile_pos <= row_pos[:, None]) & (s > 0)
    slot = relative * blocks + tile_pos * bg + inside % bg + jnp.where(is_fresh, 3 * blocks, 0)
    by_pos = slot.reshape(groups, bg, tiles)
    pick = group_order[0][:, None] == ids[None, :]
    table = jnp.sum(jnp.where(pick[:, :, None, None], by_pos[None], 0), axis=1)
    table = table.reshape(-1).astype(jnp.int32)

    dma = pltpu.SemaphoreType.DMA
    hidden = pl.pallas_call(
        functools.partial(pipeline_kernel, sections, parts, groups),
        out_shape=jax.ShapeDtypeStruct((blocks, side, width), jnp.bfloat16),
        in_specs=[
            pl.BlockSpec(memory_space=pltpu.SMEM),
            pl.BlockSpec(memory_space=pltpu.SMEM),
            pl.BlockSpec(memory_space=pltpu.VMEM),
            pl.BlockSpec(memory_space=pl.ANY),
            pl.BlockSpec(memory_space=pltpu.VMEM),
        ],
        out_specs=pl.BlockSpec(memory_space=pltpu.VMEM),
        scratch_shapes=[
            pltpu.VMEM(adjacency.shape, jnp.bfloat16),
            pltpu.VMEM((6 * blocks, side, width), jnp.bfloat16),
            pltpu.VMEM((blocks, side, width), jnp.bfloat16),
            pltpu.VMEM((blocks, side, width), jnp.bfloat16),
            pltpu.VMEM((2, blocks, side, width), jnp.bfloat16),
            dma,
            dma((2, groups)),
            dma((2, groups)),
            dma((blocks,)),
            dma((blocks,)),
            dma((2, blocks)),
            dma((2, blocks)),
        ],
        compiler_params=pltpu.CompilerParams(
            collective_id=0, has_side_effects=True, vmem_limit_bytes=56 * 2**20
        ),
    )(table, group_order[0], layer_inputs.reshape(blocks, side, width), adjacency, weights[0])

    placed = pl.pallas_call(
        place_kernel,
        out_shape=jax.ShapeDtypeStruct((blocks, side, width), jnp.bfloat16),
        grid_spec=pltpu.PrefetchScalarGridSpec(
            num_scalar_prefetch=1,
            grid=(groups,),
            in_specs=[pl.BlockSpec((bg, side, width), lambda k, o: (k, 0, 0))],
            out_specs=pl.BlockSpec((bg, side, width), lambda k, o: (o[k], 0, 0)),
        ),
    )(group_order[0], hidden)
    return placed.reshape(1, rows, width)


def solution(mesh):
    in_specs = (
        P("section", "dom", None),
        P("dom", None, None, None),
        P("dom", None),
        P("dom", None),
        P("section", None, None),
    )
    return jax.shard_map(
        functools.partial(on_device, mesh.shape["section"]),
        mesh=mesh, in_specs=in_specs, out_specs=P("section", "dom", None), check_vma=False,
    )
```

```python
import functools

import jax
import jax.numpy as jnp
from jax import lax
from jax.experimental import pallas as pl
from jax.experimental.pallas import tpu as pltpu
from jax.sharding import PartitionSpec as P

MESH = pl.DeviceIdType.MESH


def relay_plan(sections, blocks):
    far, near = blocks // 4, blocks // 8
    return ((sections - 1, 0, far), (sections - 2, far, near))


def pipeline_kernel(
    sections, parts, groups, table, order, x_ref, adj_hbm, w_ref, out_ref,
    adj, src, mine, own_land, side_land, relay_up, relay_over,
    adj_sem, stale_send, stale_recv, z_send, z_recv, f_send, f_recv,
    up_send, up_recv, over_send, over_recv, down_send, down_recv,
):
    s = lax.axis_index("section")
    d = lax.axis_index("dom")
    right, left = lax.rem(d + 1, parts), lax.rem(d + parts - 1, parts)
    blocks, side, width = x_ref.shape
    tiles = adj.shape[1]
    bg = blocks // groups
    fresh = 3 * blocks
    last = sections - 1
    odd = lax.rem(d, 2)
    across = lax.rem(d + parts - 1 + 2 * odd, parts)
    from_across = jnp.where(odd == 1, 2 * blocks, 0)
    relays = relay_plan(sections, blocks)
    relayed = sum(count for _, _, count in relays)
    direct = blocks - relayed

    load_adj = pltpu.make_async_copy(adj_hbm, adj, adj_sem)
    load_adj.start()

    for k in range(groups):
        piece = x_ref[pl.ds(order[k] * bg, bg)]
        mine[k * bg:(k + 1) * bg] = piece
        src[blocks + k * bg:blocks + (k + 1) * bg] = piece

    barrier = pltpu.get_barrier_semaphore()
    for neighbour in (left, right):
        pl.semaphore_signal(barrier, inc=1, device_id={"dom": neighbour}, device_id_type=MESH)

    @pl.when(s > 0)
    def _():
        pl.semaphore_signal(barrier, inc=1, device_id={"section": s - 1}, device_id_type=MESH)

    @pl.when(s < last)
    def _():
        pl.semaphore_signal(barrier, inc=1, device_id={"section": s + 1}, device_id_type=MESH)

    peers = 2 + jnp.where(s > 0, 1, 0) + jnp.where(s < last, 1, 0)
    for plane, _, _ in relays:
        peers = peers + jnp.where(s == 0, 1, 0) + jnp.where(s == plane, 1, 0)

        @pl.when(s == 0)
        def _():
            pl.semaphore_signal(barrier, inc=1, device_id={"section": plane}, device_id_type=MESH)

        @pl.when(s == plane)
        def _():
            pl.semaphore_signal(barrier, inc=1, device_id={"section": 0}, device_id_type=MESH)

    pl.semaphore_wait(barrier, peers)

    def stale_copy(way, k):
        base = (0 if way == 0 else 2 * blocks) + k * bg
        return pltpu.make_async_remote_copy(
            src_ref=mine.at[pl.ds(k * bg, bg)],
            dst_ref=src.at[pl.ds(base, bg)],
            send_sem=stale_send.at[way, k],
            recv_sem=stale_recv.at[way, k],
            device_id={"dom": right if way == 0 else left},
            device_id_type=MESH,
        )

    def side_copy(way, r):
        return pltpu.make_async_remote_copy(
            src_ref=own_land.at[r],
            dst_ref=side_land.at[way, r],
            send_sem=f_send.at[way, r],
            recv_sem=f_recv.at[way, r],
            device_id={"dom": right if way == 0 else left},
            device_id_type=MESH,
        )

    def up_copy(r):
        return pltpu.make_async_remote_copy(
            src_ref=out_ref.at[r],
            dst_ref=own_land.at[r],
            send_sem=z_send.at[r],
            recv_sem=z_recv.at[r],
            device_id={"section": jnp.minimum(s + 1, last)},
            device_id_type=MESH,
        )

    def partner_copy():
        return pltpu.make_async_remote_copy(
            src_ref=mine,
            dst_ref=src.at[pl.ds(jnp.where(odd == 1, 2 * blocks, 0), blocks)],
            send_sem=stale_send.at[0, 0],
            recv_sem=stale_recv.at[0, 0],
            device_id={"dom": jnp.where(odd == 1, left, right)},
            device_id_type=MESH,
        )

    def across_copy():
        return pltpu.make_async_remote_copy(
            src_ref=mine.at[pl.ds(0, direct)],
            dst_ref=src.at[pl.ds(jnp.where(odd == 1, 0, 2 * blocks), direct)],
            send_sem=stale_send.at[1, 0],
            recv_sem=stale_recv.at[1, 0],
            device_id={"dom": across},
            device_id_type=MESH,
        )

    def relay_up_copy(plane, b):
        return pltpu.make_async_remote_copy(
            src_ref=mine.at[direct + b],
            dst_ref=relay_up.at[b],
            send_sem=up_send.at[b],
            recv_sem=up_recv.at[b],
            device_id={"section": plane},
            device_id_type=MESH,
        )

    def relay_over_copy(b):
        return pltpu.make_async_remote_copy(
            src_ref=relay_up.at[b],
            dst_ref=relay_over.at[b],
            send_sem=over_send.at[b],
            recv_sem=over_recv.at[b],
            device_id={"dom": across},
            device_id_type=MESH,
        )

    def relay_down_copy(b):
        return pltpu.make_async_remote_copy(
            src_ref=relay_over.at[b],
            dst_ref=src.at[from_across + direct + b],
            send_sem=down_send.at[b],
            recv_sem=down_recv.at[b],
            device_id={"section": 0},
            device_id_type=MESH,
        )

    @pl.when(s == 0)
    def _():
        across_copy().start()
        for plane, first, count in relays:
            @pl.loop(first, first + count)
            def _(b):
                relay_up_copy(plane, b).start()

        partner_copy().start()

    for plane, first, count in relays:
        @pl.when(s == plane)
        def _():
            @pl.loop(first, first + count)
            def _(b):
                relay_up_copy(plane, b).wait_recv()
                relay_over_copy(b).start()

            for k in range(1, groups):
                for way in range(2):
                    stale_copy(way, k).start()

            @pl.loop(first, first + count)
            def _(b):
                relay_over_copy(b).wait_recv()
                relay_down_copy(b).start()

    plain = s > 0
    for plane, _, _ in relays:
        plain = plain & (s != plane)

    @pl.when(plain)
    def _():
        for k in range(1, groups):
            for way in range(2):
                stale_copy(way, k).start()

    load_adj.wait()
    own_base = jnp.where(s > 0, fresh + blocks, blocks)

    for k in range(groups):
        lo, hi = k * bg, (k + 1) * bg

        @pl.when(s > 0)
        def _():
            @pl.loop(lo, hi)
            def _(r):
                up_copy(r).wait_recv()
                side_copy(0, r).start()
                side_copy(1, r).start()

            src[fresh + blocks + lo:fresh + blocks + hi] = own_land[lo:hi]

            @pl.loop(lo, hi)
            def _(r):
                side_copy(0, r).wait_recv()
                side_copy(1, r).wait_recv()

            src[fresh + lo:fresh + hi] = side_land[0, lo:hi]
            src[fresh + 2 * blocks + lo:fresh + 2 * blocks + hi] = side_land[1, lo:hi]

        if k == 0:
            @pl.when(s == 0)
            def _():
                partner_copy().wait_recv()
                across_copy().wait_recv()

                @pl.loop(0, relayed)
                def _(b):
                    relay_down_copy(b).wait_recv()

            @pl.when(s > 0)
            def _():
                for q in range(1, groups):
                    for way in range(2):
                        stale_copy(way, q).wait_recv()

        @pl.loop(lo, hi)
        def _(r):
            row = order[k] * bg + (r - lo)
            a = jnp.concatenate([adj[row, t] for t in range(tiles)], axis=1)
            h = jnp.concatenate([src[table[r * tiles + t]] for t in range(tiles)], axis=0)
            agg = jnp.dot(a, h, preferred_element_type=jnp.float32).astype(jnp.bfloat16)
            product = jnp.dot(agg, w_ref[...], preferred_element_type=jnp.float32)
            before = src[own_base + r].astype(jnp.float32)
            out_ref[r] = (before + jnp.maximum(product, 0.0)).astype(jnp.bfloat16)

            @pl.when(s < last)
            def _():
                up_copy(r).start()

    @pl.when(s == 0)
    def _():
        partner_copy().wait_send()
        across_copy().wait_send()
        for plane, first, count in relays:
            @pl.loop(first, first + count)
            def _(b):
                relay_up_copy(plane, b).wait_send()

    for plane, first, count in relays:
        @pl.when(s == plane)
        def _():
            @pl.loop(first, first + count)
            def _(b):
                relay_over_copy(b).wait_send()
                relay_down_copy(b).wait_send()

    @pl.when(s > 0)
    def _():
        for k in range(1, groups):
            for way in range(2):
                stale_copy(way, k).wait_send()

        @pl.loop(0, blocks)
        def _(r):
            side_copy(0, r).wait_send()
            side_copy(1, r).wait_send()

    @pl.when(s < last)
    def _():
        @pl.loop(0, blocks)
        def _(r):
            up_copy(r).wait_send()


def place_kernel(groups, order, h_hbm, out_hbm, held, in_sem, out_sem):
    bg = h_hbm.shape[0] // groups

    def load(k):
        rows = pl.ds(k * bg, bg)
        return pltpu.make_async_copy(h_hbm.at[rows], held.at[rows], in_sem.at[k])

    def store(k):
        return pltpu.make_async_copy(
            held.at[pl.ds(k * bg, bg)], out_hbm.at[pl.ds(order[k] * bg, bg)], out_sem.at[k]
        )

    for k in range(groups):
        load(k).start()
    for k in range(groups):
        load(k).wait()
        store(k).start()
    for k in range(groups):
        store(k).wait()


def on_device(sections, layer_inputs, adjacency, columns, group_order, weights):
    parts = lax.axis_size("dom")
    d = lax.axis_index("dom")
    s = lax.axis_index("section")
    rows, width = layer_inputs.shape[1:]
    blocks, tiles, side = adjacency.shape[:3]
    groups = group_order.shape[1]
    bg = blocks // groups
    up = [(i, (i + 1) % parts) for i in range(parts)]
    down = [(j, i) for i, j in up]
    before = lax.ppermute(group_order, "dom", up)
    after = lax.ppermute(group_order, "dom", down)
    orders = jnp.concatenate([before, group_order, after], axis=0)
    ids = jnp.arange(groups, dtype=jnp.int32)
    position = jnp.sum(
        jnp.where(orders[:, :, None] == ids[None, None, :], ids[None, :, None], 0), axis=1
    ).astype(jnp.int32)
    relative = (columns // blocks - d + 1) % parts
    inside = columns % blocks
    key = relative * groups + inside // bg
    flat = position.reshape(-1)
    hits = key[:, :, None] == jnp.arange(3 * groups, dtype=jnp.int32)[None, None, :]
    tile_pos = jnp.sum(jnp.where(hits, flat[None, None, :], 0), axis=2)
    row_pos = jnp.repeat(position[1], bg)
    is_fresh = (tile_pos <= row_pos[:, None]) & (s > 0)
    slot = relative * blocks + tile_pos * bg + inside % bg + jnp.where(is_fresh, 3 * blocks, 0)
    by_pos = slot.reshape(groups, bg, tiles)
    pick = group_order[0][:, None] == ids[None, :]
    table = jnp.sum(jnp.where(pick[:, :, None, None], by_pos[None], 0), axis=1)
    table = table.reshape(-1).astype(jnp.int32)

    relayed = sum(count for _, _, count in relay_plan(sections, blocks))
    dma = pltpu.SemaphoreType.DMA
    hidden = pl.pallas_call(
        functools.partial(pipeline_kernel, sections, parts, groups),
        out_shape=jax.ShapeDtypeStruct((blocks, side, width), jnp.bfloat16),
        in_specs=[
            pl.BlockSpec(memory_space=pltpu.SMEM),
            pl.BlockSpec(memory_space=pltpu.SMEM),
            pl.BlockSpec(memory_space=pltpu.VMEM),
            pl.BlockSpec(memory_space=pl.ANY),
            pl.BlockSpec(memory_space=pltpu.VMEM),
        ],
        out_specs=pl.BlockSpec(memory_space=pltpu.VMEM),
        scratch_shapes=[
            pltpu.VMEM(adjacency.shape, jnp.bfloat16),
            pltpu.VMEM((6 * blocks, side, width), jnp.bfloat16),
            pltpu.VMEM((blocks, side, width), jnp.bfloat16),
            pltpu.VMEM((blocks, side, width), jnp.bfloat16),
            pltpu.VMEM((2, blocks, side, width), jnp.bfloat16),
            pltpu.VMEM((relayed, side, width), jnp.bfloat16),
            pltpu.VMEM((relayed, side, width), jnp.bfloat16),
            dma,
            dma((2, groups)),
            dma((2, groups)),
            dma((blocks,)),
            dma((blocks,)),
            dma((2, blocks)),
            dma((2, blocks)),
        ] + [dma((relayed,))] * 6,
        compiler_params=pltpu.CompilerParams(
            collective_id=0, has_side_effects=True, vmem_limit_bytes=56 * 2**20
        ),
    )(table, group_order[0], layer_inputs.reshape(blocks, side, width), adjacency, weights[0])

    placed = pl.pallas_call(
        functools.partial(place_kernel, groups),
        out_shape=jax.ShapeDtypeStruct((blocks, side, width), jnp.bfloat16),
        in_specs=[
            pl.BlockSpec(memory_space=pltpu.SMEM),
            pl.BlockSpec(memory_space=pl.ANY),
        ],
        out_specs=pl.BlockSpec(memory_space=pl.ANY),
        scratch_shapes=[
            pltpu.VMEM((blocks, side, width), jnp.bfloat16), dma((groups,)), dma((groups,)),
        ],
    )(group_order[0], hidden)
    return placed.reshape(1, rows, width)


def solution(mesh):
    in_specs = (
        P("section", "dom", None),
        P("dom", None, None, None),
        P("dom", None),
        P("dom", None),
        P("section", None, None),
    )
    return jax.shard_map(
        functools.partial(on_device, mesh.shape["section"]),
        mesh=mesh, in_specs=in_specs, out_specs=P("section", "dom", None), check_vma=False,
    )
```

```python
import functools

import jax
import jax.numpy as jnp
from jax import lax
from jax.experimental import pallas as pl
from jax.experimental.pallas import tpu as pltpu
from jax.sharding import PartitionSpec as P

MESH = pl.DeviceIdType.MESH


def relay_plan(sections, blocks):
    far, near = blocks // 4, blocks // 8
    return ((sections - 1, 0, far), (sections - 2, far, near))


def pipeline_kernel(
    sections, parts, groups, columns, own_order, order_ref, x_ref, adj_hbm, w_ref, out_ref,
    table, position, order_land, near_order, order_send, order_recv, order_local,
    adj, src, mine, own_land, side_land, relay_up, relay_over,
    adj_sem, stale_send, stale_recv, z_send, z_recv, f_send, f_recv,
    up_send, up_recv, over_send, over_recv, down_send, down_recv,
):
    s = lax.axis_index("section")
    d = lax.axis_index("dom")
    right, left = lax.rem(d + 1, parts), lax.rem(d + parts - 1, parts)
    blocks, side, width = x_ref.shape
    tiles = adj.shape[1]
    bg = blocks // groups
    fresh = 3 * blocks
    last = sections - 1
    odd = lax.rem(d, 2)
    across = lax.rem(d + parts - 1 + 2 * odd, parts)
    from_across = jnp.where(odd == 1, 2 * blocks, 0)
    relays = relay_plan(sections, blocks)
    relayed = sum(count for _, _, count in relays)
    direct = blocks - relayed

    load_adj = pltpu.make_async_copy(adj_hbm, adj, adj_sem)
    load_adj.start()

    for k in range(groups):
        piece = x_ref[pl.ds(own_order[0, k] * bg, bg)]
        mine[k * bg:(k + 1) * bg] = piece
        src[blocks + k * bg:blocks + (k + 1) * bg] = piece

    barrier = pltpu.get_barrier_semaphore()
    for neighbour in (left, right):
        pl.semaphore_signal(barrier, inc=1, device_id={"dom": neighbour}, device_id_type=MESH)

    @pl.when(s > 0)
    def _():
        pl.semaphore_signal(barrier, inc=1, device_id={"section": s - 1}, device_id_type=MESH)

    @pl.when(s < last)
    def _():
        pl.semaphore_signal(barrier, inc=1, device_id={"section": s + 1}, device_id_type=MESH)

    peers = 2 + jnp.where(s > 0, 1, 0) + jnp.where(s < last, 1, 0)
    for plane, _, _ in relays:
        peers = peers + jnp.where(s == 0, 1, 0) + jnp.where(s == plane, 1, 0)

        @pl.when(s == 0)
        def _():
            pl.semaphore_signal(barrier, inc=1, device_id={"section": plane}, device_id_type=MESH)

        @pl.when(s == plane)
        def _():
            pl.semaphore_signal(barrier, inc=1, device_id={"section": 0}, device_id_type=MESH)

    pl.semaphore_wait(barrier, peers)

    def order_copy(way):
        return pltpu.make_async_remote_copy(
            src_ref=order_ref,
            dst_ref=order_land.at[way],
            send_sem=order_send.at[way],
            recv_sem=order_recv.at[way],
            device_id={"dom": right if way == 0 else left},
            device_id_type=MESH,
        )

    for way in range(2):
        order_copy(way).start()

    def stale_copy(way, k):
        base = (0 if way == 0 else 2 * blocks) + k * bg
        return pltpu.make_async_remote_copy(
            src_ref=mine.at[pl.ds(k * bg, bg)],
            dst_ref=src.at[pl.ds(base, bg)],
            send_sem=stale_send.at[way, k],
            recv_sem=stale_recv.at[way, k],
            device_id={"dom": right if way == 0 else left},
            device_id_type=MESH,
        )

    def side_copy(way, r):
        return pltpu.make_async_remote_copy(
            src_ref=own_land.at[r],
            dst_ref=side_land.at[way, r],
            send_sem=f_send.at[way, r],
            recv_sem=f_recv.at[way, r],
            device_id={"dom": right if way == 0 else left},
            device_id_type=MESH,
        )

    def up_copy(r):
        return pltpu.make_async_remote_copy(
            src_ref=out_ref.at[r],
            dst_ref=own_land.at[r],
            send_sem=z_send.at[r],
            recv_sem=z_recv.at[r],
            device_id={"section": jnp.minimum(s + 1, last)},
            device_id_type=MESH,
        )

    def partner_copy():
        return pltpu.make_async_remote_copy(
            src_ref=mine,
            dst_ref=src.at[pl.ds(jnp.where(odd == 1, 2 * blocks, 0), blocks)],
            send_sem=stale_send.at[0, 0],
            recv_sem=stale_recv.at[0, 0],
            device_id={"dom": jnp.where(odd == 1, left, right)},
            device_id_type=MESH,
        )

    def across_copy():
        return pltpu.make_async_remote_copy(
            src_ref=mine.at[pl.ds(0, direct)],
            dst_ref=src.at[pl.ds(jnp.where(odd == 1, 0, 2 * blocks), direct)],
            send_sem=stale_send.at[1, 0],
            recv_sem=stale_recv.at[1, 0],
            device_id={"dom": across},
            device_id_type=MESH,
        )

    def relay_up_copy(plane, b):
        return pltpu.make_async_remote_copy(
            src_ref=mine.at[direct + b],
            dst_ref=relay_up.at[b],
            send_sem=up_send.at[b],
            recv_sem=up_recv.at[b],
            device_id={"section": plane},
            device_id_type=MESH,
        )

    def relay_over_copy(b):
        return pltpu.make_async_remote_copy(
            src_ref=relay_up.at[b],
            dst_ref=relay_over.at[b],
            send_sem=over_send.at[b],
            recv_sem=over_recv.at[b],
            device_id={"dom": across},
            device_id_type=MESH,
        )

    def relay_down_copy(b):
        return pltpu.make_async_remote_copy(
            src_ref=relay_over.at[b],
            dst_ref=src.at[from_across + direct + b],
            send_sem=down_send.at[b],
            recv_sem=down_recv.at[b],
            device_id={"section": 0},
            device_id_type=MESH,
        )

    @pl.when(s == 0)
    def _():
        across_copy().start()
        for plane, first, count in relays:
            @pl.loop(first, first + count)
            def _(b):
                relay_up_copy(plane, b).start()

        partner_copy().start()

    for plane, first, count in relays:
        @pl.when(s == plane)
        def _():
            @pl.loop(first, first + count)
            def _(b):
                relay_up_copy(plane, b).wait_recv()
                relay_over_copy(b).start()

            for k in range(1, groups):
                for way in range(2):
                    stale_copy(way, k).start()

            @pl.loop(first, first + count)
            def _(b):
                relay_over_copy(b).wait_recv()
                relay_down_copy(b).start()

    plain = s > 0
    for plane, _, _ in relays:
        plain = plain & (s != plane)

    @pl.when(plain)
    def _():
        for k in range(1, groups):
            for way in range(2):
                stale_copy(way, k).start()

    for way in range(2):
        order_copy(way).wait()
        local = pltpu.make_async_copy(
            order_land.at[way], near_order.at[way], order_local.at[way]
        )
        local.start()
        local.wait()

    for p in range(3):
        for g in range(groups):
            step = jnp.int32(0)
            for k in range(1, groups):
                held = own_order[0, k] if p == 1 else near_order[p // 2, 0, k]
                step = jnp.where(held == g, k, step)
            position[p * groups + g] = step

    later = s > 0

    @pl.loop(0, blocks)
    def _(r):
        k = r // bg
        row = own_order[0, k] * bg + r % bg
        for t in range(tiles):
            column = columns[row, t]
            relative = jnp.minimum(lax.rem(lax.div(column, blocks) - d + 1 + parts, parts), 2)
            inside = lax.rem(column, blocks)
            step = position[relative * groups + lax.div(inside, bg)]
            slot = relative * blocks + step * bg + lax.rem(inside, bg)
            table[r * tiles + t] = slot + jnp.where(later & (step <= k), fresh, 0)

    load_adj.wait()
    own_base = jnp.where(s > 0, fresh + blocks, blocks)

    for k in range(groups):
        lo, hi = k * bg, (k + 1) * bg

        @pl.when(s > 0)
        def _():
            @pl.loop(lo, hi)
            def _(r):
                up_copy(r).wait_recv()
                side_copy(0, r).start()
                side_copy(1, r).start()

            src[fresh + blocks + lo:fresh + blocks + hi] = own_land[lo:hi]

            @pl.loop(lo, hi)
            def _(r):
                side_copy(0, r).wait_recv()
                side_copy(1, r).wait_recv()

            src[fresh + lo:fresh + hi] = side_land[0, lo:hi]
            src[fresh + 2 * blocks + lo:fresh + 2 * blocks + hi] = side_land[1, lo:hi]

        if k == 0:
            @pl.when(s == 0)
            def _():
                partner_copy().wait_recv()
                across_copy().wait_recv()

                @pl.loop(0, relayed)
                def _(b):
                    relay_down_copy(b).wait_recv()

            @pl.when(s > 0)
            def _():
                for q in range(1, groups):
                    for way in range(2):
                        stale_copy(way, q).wait_recv()

        @pl.loop(lo, hi)
        def _(r):
            row = own_order[0, k] * bg + (r - lo)
            a = jnp.concatenate([adj[row, t] for t in range(tiles)], axis=1)
            h = jnp.concatenate([src[table[r * tiles + t]] for t in range(tiles)], axis=0)
            agg = jnp.dot(a, h, preferred_element_type=jnp.float32).astype(jnp.bfloat16)
            product = jnp.dot(agg, w_ref[...], preferred_element_type=jnp.float32)
            before = src[own_base + r].astype(jnp.float32)
            out_ref[r] = (before + jnp.maximum(product, 0.0)).astype(jnp.bfloat16)

            @pl.when(s < last)
            def _():
                up_copy(r).start()

    @pl.when(s == 0)
    def _():
        partner_copy().wait_send()
        across_copy().wait_send()
        for plane, first, count in relays:
            @pl.loop(first, first + count)
            def _(b):
                relay_up_copy(plane, b).wait_send()

    for plane, first, count in relays:
        @pl.when(s == plane)
        def _():
            @pl.loop(first, first + count)
            def _(b):
                relay_over_copy(b).wait_send()
                relay_down_copy(b).wait_send()

    @pl.when(s > 0)
    def _():
        for k in range(1, groups):
            for way in range(2):
                stale_copy(way, k).wait_send()

        @pl.loop(0, blocks)
        def _(r):
            side_copy(0, r).wait_send()
            side_copy(1, r).wait_send()

    @pl.when(s < last)
    def _():
        @pl.loop(0, blocks)
        def _(r):
            up_copy(r).wait_send()


def place_kernel(groups, order, h_hbm, out_hbm, held, in_sem, out_sem):
    bg = h_hbm.shape[0] // groups

    def load(k):
        rows = pl.ds(k * bg, bg)
        return pltpu.make_async_copy(h_hbm.at[rows], held.at[rows], in_sem.at[k])

    def store(k):
        return pltpu.make_async_copy(
            held.at[pl.ds(k * bg, bg)], out_hbm.at[pl.ds(order[k] * bg, bg)], out_sem.at[k]
        )

    for k in range(groups):
        load(k).start()
    for k in range(groups):
        load(k).wait()
        store(k).start()
    for k in range(groups):
        store(k).wait()


def on_device(sections, layer_inputs, adjacency, columns, group_order, weights):
    parts = lax.axis_size("dom")
    rows, width = layer_inputs.shape[1:]
    blocks, tiles, side = adjacency.shape[:3]
    groups = group_order.shape[1]
    relayed = sum(count for _, _, count in relay_plan(sections, blocks))
    dma = pltpu.SemaphoreType.DMA
    hidden = pl.pallas_call(
        functools.partial(pipeline_kernel, sections, parts, groups),
        out_shape=jax.ShapeDtypeStruct((blocks, side, width), jnp.bfloat16),
        in_specs=[
            pl.BlockSpec(memory_space=pltpu.SMEM),
            pl.BlockSpec(memory_space=pltpu.SMEM),
            pl.BlockSpec(memory_space=pltpu.VMEM),
            pl.BlockSpec(memory_space=pltpu.VMEM),
            pl.BlockSpec(memory_space=pl.ANY),
            pl.BlockSpec(memory_space=pltpu.VMEM),
        ],
        out_specs=pl.BlockSpec(memory_space=pltpu.VMEM),
        scratch_shapes=[
            pltpu.SMEM((blocks * tiles,), jnp.int32),
            pltpu.SMEM((3 * groups,), jnp.int32),
            pltpu.VMEM((2, 1, groups), jnp.int32),
            pltpu.SMEM((2, 1, groups), jnp.int32),
            dma((2,)),
            dma((2,)),
            dma((2,)),
            pltpu.VMEM(adjacency.shape, jnp.bfloat16),
            pltpu.VMEM((6 * blocks, side, width), jnp.bfloat16),
            pltpu.VMEM((blocks, side, width), jnp.bfloat16),
            pltpu.VMEM((blocks, side, width), jnp.bfloat16),
            pltpu.VMEM((2, blocks, side, width), jnp.bfloat16),
            pltpu.VMEM((relayed, side, width), jnp.bfloat16),
            pltpu.VMEM((relayed, side, width), jnp.bfloat16),
            dma,
            dma((2, groups)),
            dma((2, groups)),
            dma((blocks,)),
            dma((blocks,)),
            dma((2, blocks)),
            dma((2, blocks)),
        ] + [dma((relayed,))] * 6,
        compiler_params=pltpu.CompilerParams(
            collective_id=0, has_side_effects=True, vmem_limit_bytes=56 * 2**20
        ),
    )(
        columns, group_order, group_order,
        layer_inputs.reshape(blocks, side, width), adjacency, weights[0],
    )

    placed = pl.pallas_call(
        functools.partial(place_kernel, groups),
        out_shape=jax.ShapeDtypeStruct((blocks, side, width), jnp.bfloat16),
        in_specs=[
            pl.BlockSpec(memory_space=pltpu.SMEM),
            pl.BlockSpec(memory_space=pl.ANY),
        ],
        out_specs=pl.BlockSpec(memory_space=pl.ANY),
        scratch_shapes=[
            pltpu.VMEM((blocks, side, width), jnp.bfloat16), dma((groups,)), dma((groups,)),
        ],
    )(group_order[0], hidden)
    return placed.reshape(1, rows, width)


def solution(mesh):
    in_specs = (
        P("section", "dom", None),
        P("dom", None, None, None),
        P("dom", None),
        P("dom", None),
        P("section", None, None),
    )
    return jax.shard_map(
        functools.partial(on_device, mesh.shape["section"]),
        mesh=mesh, in_specs=in_specs, out_specs=P("section", "dom", None), check_vma=False,
    )
```

```python
import functools

import jax
import jax.numpy as jnp
from jax import lax
from jax.experimental import pallas as pl
from jax.experimental.pallas import tpu as pltpu
from jax.sharding import PartitionSpec as P

MESH = pl.DeviceIdType.MESH


def relay_plan(sections, blocks):
    far, near = blocks // 4, blocks // 8
    return ((sections - 1, 0, far), (sections - 2, far, near))


def pipeline_kernel(
    sections, parts, groups, columns, own_order, order_ref, x_ref, adj_hbm, w_ref, out_ref,
    table, position, order_land, near_order, order_send, order_recv, order_local,
    adj, src, mine, own_land, side_land, relay_up, relay_over,
    adj_sem, stale_send, stale_recv, z_send, z_recv, f_send, f_recv,
    up_send, up_recv, over_send, over_recv, down_send, down_recv,
):
    s = lax.axis_index("section")
    d = lax.axis_index("dom")
    right, left = lax.rem(d + 1, parts), lax.rem(d + parts - 1, parts)
    blocks, side, width = x_ref.shape
    tiles = adj.shape[1]
    bg = blocks // groups
    fresh = 3 * blocks
    last = sections - 1
    odd = lax.rem(d, 2)
    across = lax.rem(d + parts - 1 + 2 * odd, parts)
    from_across = jnp.where(odd == 1, 2 * blocks, 0)
    relays = relay_plan(sections, blocks)
    relayed = sum(count for _, _, count in relays)
    direct = blocks - relayed

    load_adj = pltpu.make_async_copy(adj_hbm, adj, adj_sem)
    load_adj.start()

    for k in range(groups):
        piece = x_ref[pl.ds(own_order[0, k] * bg, bg)]
        mine[k * bg:(k + 1) * bg] = piece
        src[blocks + k * bg:blocks + (k + 1) * bg] = piece

    barrier = pltpu.get_barrier_semaphore()
    for neighbour in (left, right):
        pl.semaphore_signal(barrier, inc=1, device_id={"dom": neighbour}, device_id_type=MESH)

    @pl.when(s > 0)
    def _():
        pl.semaphore_signal(barrier, inc=1, device_id={"section": s - 1}, device_id_type=MESH)

    @pl.when(s < last)
    def _():
        pl.semaphore_signal(barrier, inc=1, device_id={"section": s + 1}, device_id_type=MESH)

    peers = 2 + jnp.where(s > 0, 1, 0) + jnp.where(s < last, 1, 0)
    for plane, _, _ in relays:
        peers = peers + jnp.where(s == 0, 1, 0) + jnp.where(s == plane, 1, 0)

        @pl.when(s == 0)
        def _():
            pl.semaphore_signal(barrier, inc=1, device_id={"section": plane}, device_id_type=MESH)

        @pl.when(s == plane)
        def _():
            pl.semaphore_signal(barrier, inc=1, device_id={"section": 0}, device_id_type=MESH)

    pl.semaphore_wait(barrier, peers)

    def order_copy(way):
        return pltpu.make_async_remote_copy(
            src_ref=order_ref,
            dst_ref=order_land.at[way],
            send_sem=order_send.at[way],
            recv_sem=order_recv.at[way],
            device_id={"dom": right if way == 0 else left},
            device_id_type=MESH,
        )

    for way in range(2):
        order_copy(way).start()

    def stale_copy(way, k):
        base = (0 if way == 0 else 2 * blocks) + k * bg
        return pltpu.make_async_remote_copy(
            src_ref=mine.at[pl.ds(k * bg, bg)],
            dst_ref=src.at[pl.ds(base, bg)],
            send_sem=stale_send.at[way, k],
            recv_sem=stale_recv.at[way, k],
            device_id={"dom": right if way == 0 else left},
            device_id_type=MESH,
        )

    def side_copy(way, r):
        return pltpu.make_async_remote_copy(
            src_ref=own_land.at[r],
            dst_ref=side_land.at[way, r],
            send_sem=f_send.at[way, r],
            recv_sem=f_recv.at[way, r],
            device_id={"dom": right if way == 0 else left},
            device_id_type=MESH,
        )

    def up_copy(r):
        return pltpu.make_async_remote_copy(
            src_ref=out_ref.at[r],
            dst_ref=own_land.at[r],
            send_sem=z_send.at[r],
            recv_sem=z_recv.at[r],
            device_id={"section": jnp.minimum(s + 1, last)},
            device_id_type=MESH,
        )

    def partner_copy():
        return pltpu.make_async_remote_copy(
            src_ref=mine,
            dst_ref=src.at[pl.ds(jnp.where(odd == 1, 2 * blocks, 0), blocks)],
            send_sem=stale_send.at[0, 0],
            recv_sem=stale_recv.at[0, 0],
            device_id={"dom": jnp.where(odd == 1, left, right)},
            device_id_type=MESH,
        )

    def across_copy():
        return pltpu.make_async_remote_copy(
            src_ref=mine.at[pl.ds(0, direct)],
            dst_ref=src.at[pl.ds(jnp.where(odd == 1, 0, 2 * blocks), direct)],
            send_sem=stale_send.at[1, 0],
            recv_sem=stale_recv.at[1, 0],
            device_id={"dom": across},
            device_id_type=MESH,
        )

    def relay_up_copy(plane, b):
        return pltpu.make_async_remote_copy(
            src_ref=mine.at[direct + b],
            dst_ref=relay_up.at[b],
            send_sem=up_send.at[b],
            recv_sem=up_recv.at[b],
            device_id={"section": plane},
            device_id_type=MESH,
        )

    def relay_over_copy(b):
        return pltpu.make_async_remote_copy(
            src_ref=relay_up.at[b],
            dst_ref=relay_over.at[b],
            send_sem=over_send.at[b],
            recv_sem=over_recv.at[b],
            device_id={"dom": across},
            device_id_type=MESH,
        )

    def relay_down_copy(b):
        return pltpu.make_async_remote_copy(
            src_ref=relay_over.at[b],
            dst_ref=src.at[from_across + direct + b],
            send_sem=down_send.at[b],
            recv_sem=down_recv.at[b],
            device_id={"section": 0},
            device_id_type=MESH,
        )

    def forward(r):
        up_copy(r).wait_recv()
        side_copy(0, r).start()
        side_copy(1, r).start()

    @pl.when(s == 0)
    def _():
        across_copy().start()
        for plane, first, count in relays:
            @pl.loop(first, first + count)
            def _(b):
                relay_up_copy(plane, b).start()

        partner_copy().start()

    for plane, first, count in relays:
        @pl.when(s == plane)
        def _():
            @pl.loop(first, first + count)
            def _(b):
                relay_up_copy(plane, b).wait_recv()
                relay_over_copy(b).start()

            for k in range(1, groups):
                for way in range(2):
                    stale_copy(way, k).start()

            @pl.loop(first, first + count)
            def _(b):
                relay_over_copy(b).wait_recv()
                relay_down_copy(b).start()

    plain = s > 0
    for plane, _, _ in relays:
        plain = plain & (s != plane)

    @pl.when(plain)
    def _():
        for k in range(1, groups):
            for way in range(2):
                stale_copy(way, k).start()

    for way in range(2):
        order_copy(way).wait()
        local = pltpu.make_async_copy(
            order_land.at[way], near_order.at[way], order_local.at[way]
        )
        local.start()
        local.wait()

    for p in range(3):
        for g in range(groups):
            step = jnp.int32(0)
            for k in range(1, groups):
                held = own_order[0, k] if p == 1 else near_order[p // 2, 0, k]
                step = jnp.where(held == g, k, step)
            position[p * groups + g] = step

    later = s > 0

    @pl.loop(0, blocks)
    def _(r):
        k = r // bg
        row = own_order[0, k] * bg + r % bg
        for t in range(tiles):
            column = columns[row, t]
            relative = jnp.minimum(lax.rem(lax.div(column, blocks) - d + 1 + parts, parts), 2)
            inside = lax.rem(column, blocks)
            step = position[relative * groups + lax.div(inside, bg)]
            slot = relative * blocks + step * bg + lax.rem(inside, bg)
            table[r * tiles + t] = slot + jnp.where(later & (step <= k), fresh, 0)

    load_adj.wait()
    own_base = jnp.where(s > 0, fresh + blocks, blocks)

    for k in range(groups):
        lo, hi = k * bg, (k + 1) * bg

        @pl.when(s > 0)
        def _():
            if k == 0:
                @pl.loop(lo, hi)
                def _(r):
                    forward(r)

            src[fresh + blocks + lo:fresh + blocks + hi] = own_land[lo:hi]

            @pl.loop(lo, hi)
            def _(r):
                side_copy(0, r).wait_recv()
                side_copy(1, r).wait_recv()

            src[fresh + lo:fresh + hi] = side_land[0, lo:hi]
            src[fresh + 2 * blocks + lo:fresh + 2 * blocks + hi] = side_land[1, lo:hi]

        if k == 0:
            @pl.when(s == 0)
            def _():
                partner_copy().wait_recv()
                across_copy().wait_recv()

                @pl.loop(0, relayed)
                def _(b):
                    relay_down_copy(b).wait_recv()

            @pl.when(s > 0)
            def _():
                for q in range(1, groups):
                    for way in range(2):
                        stale_copy(way, q).wait_recv()

        @pl.loop(lo, hi)
        def _(r):
            if k + 1 < groups:
                @pl.when(s > 0)
                def _():
                    forward(r + bg)

            row = own_order[0, k] * bg + (r - lo)
            a = jnp.concatenate([adj[row, t] for t in range(tiles)], axis=1)
            h = jnp.concatenate([src[table[r * tiles + t]] for t in range(tiles)], axis=0)
            agg = jnp.dot(a, h, preferred_element_type=jnp.float32).astype(jnp.bfloat16)
            product = jnp.dot(agg, w_ref[...], preferred_element_type=jnp.float32)
            before = src[own_base + r].astype(jnp.float32)
            out_ref[r] = (before + jnp.maximum(product, 0.0)).astype(jnp.bfloat16)

            @pl.when(s < last)
            def _():
                up_copy(r).start()

    @pl.when(s == 0)
    def _():
        partner_copy().wait_send()
        across_copy().wait_send()
        for plane, first, count in relays:
            @pl.loop(first, first + count)
            def _(b):
                relay_up_copy(plane, b).wait_send()

    for plane, first, count in relays:
        @pl.when(s == plane)
        def _():
            @pl.loop(first, first + count)
            def _(b):
                relay_over_copy(b).wait_send()
                relay_down_copy(b).wait_send()

    @pl.when(s > 0)
    def _():
        for k in range(1, groups):
            for way in range(2):
                stale_copy(way, k).wait_send()

        @pl.loop(0, blocks)
        def _(r):
            side_copy(0, r).wait_send()
            side_copy(1, r).wait_send()

    @pl.when(s < last)
    def _():
        @pl.loop(0, blocks)
        def _(r):
            up_copy(r).wait_send()


def place_kernel(groups, order, h_hbm, out_hbm, held, in_sem, out_sem):
    bg = h_hbm.shape[0] // groups

    def load(k):
        rows = pl.ds(k * bg, bg)
        return pltpu.make_async_copy(h_hbm.at[rows], held.at[rows], in_sem.at[k])

    def store(k):
        return pltpu.make_async_copy(
            held.at[pl.ds(k * bg, bg)], out_hbm.at[pl.ds(order[k] * bg, bg)], out_sem.at[k]
        )

    for k in range(groups):
        load(k).start()
    for k in range(groups):
        load(k).wait()
        store(k).start()
    for k in range(groups):
        store(k).wait()


def on_device(sections, layer_inputs, adjacency, columns, group_order, weights):
    parts = lax.axis_size("dom")
    rows, width = layer_inputs.shape[1:]
    blocks, tiles, side = adjacency.shape[:3]
    groups = group_order.shape[1]
    relayed = sum(count for _, _, count in relay_plan(sections, blocks))
    dma = pltpu.SemaphoreType.DMA
    hidden = pl.pallas_call(
        functools.partial(pipeline_kernel, sections, parts, groups),
        out_shape=jax.ShapeDtypeStruct((blocks, side, width), jnp.bfloat16),
        in_specs=[
            pl.BlockSpec(memory_space=pltpu.SMEM),
            pl.BlockSpec(memory_space=pltpu.SMEM),
            pl.BlockSpec(memory_space=pltpu.VMEM),
            pl.BlockSpec(memory_space=pltpu.VMEM),
            pl.BlockSpec(memory_space=pl.ANY),
            pl.BlockSpec(memory_space=pltpu.VMEM),
        ],
        out_specs=pl.BlockSpec(memory_space=pltpu.VMEM),
        scratch_shapes=[
            pltpu.SMEM((blocks * tiles,), jnp.int32),
            pltpu.SMEM((3 * groups,), jnp.int32),
            pltpu.VMEM((2, 1, groups), jnp.int32),
            pltpu.SMEM((2, 1, groups), jnp.int32),
            dma((2,)),
            dma((2,)),
            dma((2,)),
            pltpu.VMEM(adjacency.shape, jnp.bfloat16),
            pltpu.VMEM((6 * blocks, side, width), jnp.bfloat16),
            pltpu.VMEM((blocks, side, width), jnp.bfloat16),
            pltpu.VMEM((blocks, side, width), jnp.bfloat16),
            pltpu.VMEM((2, blocks, side, width), jnp.bfloat16),
            pltpu.VMEM((relayed, side, width), jnp.bfloat16),
            pltpu.VMEM((relayed, side, width), jnp.bfloat16),
            dma,
            dma((2, groups)),
            dma((2, groups)),
            dma((blocks,)),
            dma((blocks,)),
            dma((2, blocks)),
            dma((2, blocks)),
        ] + [dma((relayed,))] * 6,
        compiler_params=pltpu.CompilerParams(
            collective_id=0, has_side_effects=True, vmem_limit_bytes=56 * 2**20
        ),
    )(
        columns, group_order, group_order,
        layer_inputs.reshape(blocks, side, width), adjacency, weights[0],
    )

    placed = pl.pallas_call(
        functools.partial(place_kernel, groups),
        out_shape=jax.ShapeDtypeStruct((blocks, side, width), jnp.bfloat16),
        in_specs=[
            pl.BlockSpec(memory_space=pltpu.SMEM),
            pl.BlockSpec(memory_space=pl.ANY),
        ],
        out_specs=pl.BlockSpec(memory_space=pl.ANY),
        scratch_shapes=[
            pltpu.VMEM((blocks, side, width), jnp.bfloat16), dma((groups,)), dma((groups,)),
        ],
    )(group_order[0], hidden)
    return placed.reshape(1, rows, width)


def solution(mesh):
    in_specs = (
        P("section", "dom", None),
        P("dom", None, None, None),
        P("dom", None),
        P("dom", None),
        P("section", None, None),
    )
    return jax.shard_map(
        functools.partial(on_device, mesh.shape["section"]),
        mesh=mesh, in_specs=in_specs, out_specs=P("section", "dom", None), check_vma=False,
    )
```
